32 devices in a mesh: layer: 8 (over z, x), split: 4 (over y, core).
Axes of the slice: x: 2, y: 2, z: 4, core: 2. Of those that a mesh axis runs over, the one named last changes fastest.
Arguments:
- right_side: float32 [32, 512, 128], P('layer', 'split'), may hold values from -6 to 6
- diagonal: float32 [32, 512, 128], P('layer', 'split'), may hold values from 0.1 to 1
- inverses: float32 [32, 512, 512], P('layer', None, 'split'), may hold values from -1 to 1, as said below
Outputs:
- solution_field: float32 [32, 512, 128], P('layer', 'split')
- residual: float32 [32, 512, 128], P('layer', 'split')
The draws below stay inside these ranges and needn't reach their ends.
Inputs may be any that keep to these rules, and one draw needn't show every extreme that they name: `inverses`: each plane's inverse is a diagonal matrix with entries between 0.5 and 1 plus a dense coupling with zero diagonal and spectral norm below 0.2.
All inputs are finite; a program needn't handle non-finite values.
Results may differ from the reference program's by a relative error of at most 0.0003.
Values sent between devices are 32-bit elements; how exact they have to be, the bound alone decides.
No kernel may reach another device: no remote copies, remote signals or barrier semaphores. Data moves between devices by JAX's collectives and lax.ppermute only.
A program may use at most 64 MiB of HBM per device.

```python
import jax
import jax.numpy as jnp
from jax import lax

NX = 512
NY = 128
SHEET_TOTAL = 32


def draw_inverses(key, part):
    speed_seed, sheet_seed, pulse_seed, linkage_seed = jax.random.split(jax.random.fold_in(key, 11), 4)
    low_rate = jnp.log(0.5 / SHEET_TOTAL)
    high_rate = jnp.log(1.0 / 30.0)
    base_rate = jnp.exp(jax.random.uniform(speed_seed, (1, NX), jnp.float32, low_rate, high_rate))
    plane_factor = jax.random.uniform(sheet_seed, (SHEET_TOTAL, 1), jnp.float32, 0.6, 1.4)
    retained_share = jnp.exp(-base_rate * plane_factor)
    pulse_batches = jax.random.uniform(pulse_seed, (SHEET_TOTAL, 1), jnp.float32) < 6.0 / SHEET_TOTAL
    retained_share = jnp.where(pulse_batches, 0.6 * retained_share, retained_share)
    coupling = jax.random.normal(linkage_seed, (SHEET_TOTAL, NX, NX), jnp.float32) * (0.05 / jnp.sqrt(1.0 * NX))
    identity = jnp.eye(NX, dtype=jnp.float32)[None, :, :]
    coupling = coupling * (1.0 - identity)
    return coupling + retained_share[:, :, None] * identity


def block_scale(own_key, extent, shards, smallest, high):
    def one(axis_at, parts):
        steps = jax.random.uniform(jax.random.fold_in(jax.random.fold_in(own_key, 6), axis_at), (parts,), jnp.float32, smallest / len(shards), high / len(shards))
        return jnp.repeat(jnp.exp(steps), extent[axis_at] // parts).reshape((-1,) + (1,) * (len(extent) - axis_at - 1))

    level = one(*shards[0])
    for cut in shards[1:]:
        level = level * one(*cut)
    return level


def gaussian(stream_key, dims, deviation, limit, shards=(), kind=jnp.bfloat16):
    gain = block_scale(stream_key, dims, shards, -0.22, 0.18) if shards else 1.0
    values = jax.random.normal(stream_key, dims, jnp.float32) * deviation * gain
    return jnp.minimum(jnp.maximum(values, -limit), limit).astype(kind)


def setup_inputs(seed: int = 0) -> dict:
    key_list = jax.random.split(jax.random.key(seed), 4)
    right_side = gaussian(key_list[0], (SHEET_TOTAL, NX, NY), 1.0, 6.0, ((0, 8), (1, 4)), jnp.float32)
    diagonal = jnp.clip(0.1 + 0.9 * jax.random.uniform(key_list[1], (SHEET_TOTAL, NX, NY), jnp.float32) ** block_scale(key_list[1], (SHEET_TOTAL, NX, NY), ((0, 8), (1, 4)), -0.2, 0.2), 0.1, 1.0)
    inverses = draw_inverses(jax.random.fold_in(key_list[3], 71), 0)
    return {"right_side": right_side, "diagonal": diagonal, "inverses": inverses}


def stencil(values, diagonal):
    padded = jnp.pad(values, 1)
    beside = padded[2:, 1:-1, 1:-1] + padded[:-2, 1:-1, 1:-1]
    beside = beside + padded[1:-1, 2:, 1:-1] + padded[1:-1, :-2, 1:-1]
    beside = beside + padded[1:-1, 1:-1, 2:] + padded[1:-1, 1:-1, :-2]
    return (6.0 + diagonal) * values - beside


def reference(right_side, diagonal, inverses):
    highest = lax.Precision.HIGHEST

    def down_plane(carried, inputs):
        matrix, source = inputs
        carried = jnp.dot(matrix, source + carried, precision=highest)
        return carried, carried

    start = jnp.zeros((NX, NY), jnp.float32)
    _, lower_sweep = lax.scan(down_plane, start, (inverses, right_side))

    def up_plane(carried, inputs):
        matrix, below = inputs
        summed = below + jnp.dot(matrix, carried, precision=highest)
        return summed, summed

    _, direction = lax.scan(up_plane, start, (inverses, lower_sweep), reverse=True)
    image = stencil(direction, diagonal)
    step_alpha = jnp.sum(right_side * right_side) / jnp.sum(right_side * image)
    middle = right_side - step_alpha * image
    tangent = stencil(middle, diagonal)
    step_omega = jnp.sum(tangent * middle) / jnp.sum(tangent * tangent)
    return step_alpha * direction + step_omega * middle, middle - step_omega * tangent
```

```python
import jax
import jax.numpy as jnp
from jax import lax
from jax.experimental import pallas as pl
from jax.experimental.pallas import tpu as pltpu
from jax.sharding import PartitionSpec as P

F32 = jnp.float32
BF16 = jnp.bfloat16
EDGE = 8


def split_parts(x):
    high = x.astype(BF16)
    return high, (x - high.astype(F32)).astype(BF16)


def dot_nt(a, b):
    return lax.dot_general(a, b, (((1,), (1,)), ((), ())), preferred_element_type=F32)


def apply_rows(rows, high, low):
    n = rows.shape[0]
    a, b = split_parts(rows)
    both = dot_nt(jnp.concatenate([a, b], axis=0), high)
    return both[:n] + both[n:] + dot_nt(a, low)


def product(a, b):
    ah, al = a
    bh, bl = b
    out = jnp.dot(ah, bh, preferred_element_type=F32)
    out = out + jnp.dot(ah, bl, preferred_element_type=F32)
    return out + jnp.dot(al, bh, preferred_element_type=F32)


def chain_product(pairs):
    while len(pairs) > 1:
        merged = [
            split_parts(product(pairs[i], pairs[i + 1])) for i in range(0, len(pairs) - 1, 2)
        ]
        if len(pairs) % 2:
            merged.append(pairs[-1])
        pairs = merged
    return pairs[0]


def call(body, out, *args, smem=0):
    vm = pl.BlockSpec(memory_space=pltpu.VMEM)
    specs = [pl.BlockSpec(memory_space=pltpu.SMEM)] * smem + [vm] * (len(args) - smem)
    shapes = [jax.ShapeDtypeStruct(s, d) for s, d in out]
    return pl.pallas_call(
        body, out_shape=shapes, in_specs=specs, out_specs=[vm] * len(shapes), name=body.__name__
    )(*args)


def prepare(place, *refs):
    count = place.shape[0]
    blocks = refs[:count]
    pieces, mh, ml, ph, plo, qh, qlo, tail, cols = refs[count:]
    planes, nx, width = blocks[0].shape
    for j in range(count):
        at = pl.multiple_of(place[j] * width, width)
        for k in range(planes):
            high, low = split_parts(blocks[j][k])
            mh[k, :, pl.ds(at, width)] = high
            ml[k, :, pl.ds(at, width)] = low
        cols[:, :, j * width : (j + 1) * width] = pieces[j]
    state = cols[0]
    for k in range(planes):
        if k:
            state = state + cols[k]
        state = apply_rows(state, mh[k], ml[k])
    tail[...] = state
    order = [(mh[k], ml[k]) for k in range(planes)]
    ph[...], plo[...] = chain_product(order[::-1])
    qh[...], qlo[...] = chain_product(order)


def hop(held, came, base, high, low, now, out):
    state = held[...] + came[...]
    now[...] = state
    out[...] = base[...] + apply_rows(state, high[...], low[...])


def turn(held, came, cols, mh, ml, lower, top):
    planes = cols.shape[0]
    state = held[...] + came[...]
    for k in range(planes):
        state = apply_rows(cols[k] + state, mh[k], ml[k])
        lower[k] = state
    for k in reversed(range(planes - 1)):
        state = lower[k] + apply_rows(state, mh[k], ml[k])
    top[...] = state


def rise(held, came, lower, mh, ml, direction, now):
    planes = lower.shape[0]
    state = held[...] + came[...]
    now[...] = state
    for k in reversed(range(planes)):
        state = lower[k] + apply_rows(state, mh[k], ml[k])
        direction[k] = state


def pack(direction, behind, above, ahead, out, tall):
    planes, ny, nx = direction.shape
    extended = jnp.concatenate([behind[...], direction[...], above[...][None], ahead[...]], axis=0)
    flat = extended.reshape((planes + 4) * ny, nx)
    tall[:EDGE] = jnp.zeros((EDGE, tall.shape[1]), F32)
    tall[EDGE + nx :] = jnp.zeros((EDGE, tall.shape[1]), F32)
    tall[EDGE : EDGE + nx] = flat.T
    count = out.shape[0]
    width = nx // count
    for j in range(count):
        out[j] = tall[j * width : j * width + width + 2 * EDGE]


def plane_stencil(below, here, above, diagonal):
    rows, ny = here.shape
    lane = lax.broadcasted_iota(jnp.int32, here.shape, 1)
    beside = below + above + pltpu.roll(here, 1, 0) + pltpu.roll(here, rows - 1, 0)
    beside = beside + jnp.where(lane > 0, pltpu.roll(here, 1, 1), 0.0)
    beside = beside + jnp.where(lane < ny - 1, pltpu.roll(here, ny - 1, 1), 0.0)
    return (6.0 + diagonal) * here - beside


def apply_rhs(extended, out):
    planes = out.shape[0]
    for k in range(planes):
        value = plane_stencil(
            extended[0, k], extended[0, k + 1], extended[0, k + 2], extended[1, k + 1]
        )
        out[k] = value[EDGE:-EDGE]


def images(where, recv, extended, applied_rhs, direction, image, applied_image, sums):
    planes = direction.shape[0]
    count, rows, packed = recv.shape
    part = packed // (planes + 4)
    depth = [
        jnp.concatenate([recv[j, :, p * part : (p + 1) * part] for j in range(count)], axis=1)
        for p in range(planes + 4)
    ]
    row = lax.broadcasted_iota(jnp.int32, depth[0].shape, 0) + where[0]
    inside_x = jnp.logical_and(row >= 0, row < where[2])
    made = {}
    for p in range(1, planes + 3):
        value = plane_stencil(depth[p - 1], depth[p], depth[p + 1], extended[1, p - 1])
        at = where[1] + p
        inside_z = jnp.logical_and(at >= 0, at < where[3])
        made[p] = jnp.where(jnp.logical_and(inside_x, inside_z), value, 0.0)
    totals = [jnp.zeros((EDGE, depth[0].shape[1]), F32) for _ in range(8)]
    for k in range(planes):
        p = k + 2
        twice = plane_stencil(made[p - 1], made[p], made[p + 1], extended[1, k + 1])[EDGE:-EDGE]
        once = made[p][EDGE:-EDGE]
        source = extended[0, k + 1][EDGE:-EDGE]
        about = applied_rhs[k]
        direction[k] = depth[p][EDGE:-EDGE]
        image[k] = once
        applied_image[k] = twice
        terms = (
            source * source,
            source * once,
            about * source,
            about * once + twice * source,
            twice * once,
            about * about,
            about * twice,
            twice * twice,
        )
        for i, term in enumerate(terms):
            totals[i] = totals[i] + jnp.sum(term.reshape(-1, EDGE, term.shape[1]), axis=0)
    lane = lax.broadcasted_iota(jnp.int32, sums.shape, 1)
    line = jnp.zeros(sums.shape, F32)
    for i, total in enumerate(totals):
        line = jnp.where(lane == i, jnp.sum(total), line)
    sums[...] = line


def finish(every, direction, image, applied_image, right_side, applied_rhs, solved, residual):
    total = jnp.sum(every[...], axis=0, keepdims=True)
    lane = lax.broadcasted_iota(jnp.int32, total.shape, 1)

    def pick(i):
        return jnp.sum(jnp.where(lane == i, total, 0.0), axis=1, keepdims=True)

    rr, ri, ar, cross, aii, arar, arai, aiai = [pick(i) for i in range(8)]
    alpha = rr / ri
    upper = ar - alpha * cross + alpha * alpha * aii
    under = arar - 2.0 * alpha * arai + alpha * alpha * aiai
    omega = upper / under
    for k in range(direction.shape[0]):
        middle = right_side[k] - alpha * image[k]
        tangent = applied_rhs[k] - alpha * applied_image[k]
        solved[k] = alpha * direction[k] + omega * middle
        residual[k] = middle - omega * tangent


def neighbours(x, axis):
    size = lax.axis_size(axis)
    up = [(i, i + 1) for i in range(size - 1)]
    down = [(i + 1, i) for i in range(size - 1)]
    return up, down


def per_device(right_side, diagonal, inverses):
    splits = lax.axis_size("split")
    depth = lax.axis_size("layer")
    own = lax.axis_index("split")
    layer = lax.axis_index("layer")
    planes, width, ny = right_side.shape
    nx = inverses.shape[1]
    part = ny // splits

    blocks = [inverses]
    offsets = [0]
    step = splits // 2
    while step:
        route = [(i, i ^ step) for i in range(splits)]
        blocks = blocks + [lax.ppermute(b, "split", route) for b in blocks]
        offsets = offsets + [o ^ step for o in offsets]
        step //= 2
    place = jnp.stack([own ^ o for o in offsets]).astype(jnp.int32)

    turned = jnp.swapaxes(right_side, 1, 2).reshape(planes, splits, part, width)
    pieces = lax.all_to_all(
        jnp.swapaxes(turned, 0, 1), "split", split_axis=0, concat_axis=0, tiled=True
    )

    pair = jnp.stack([right_side, diagonal])
    up, down = neighbours(pair, "layer")
    before = lax.ppermute(pair[:, -1:], "layer", up)
    after = lax.ppermute(pair[:, :1], "layer", down)
    pair = jnp.concatenate([before, pair, after], axis=1)
    up, down = neighbours(pair, "split")
    before = lax.ppermute(pair[:, :, -EDGE:], "split", up)
    after = lax.ppermute(pair[:, :, :EDGE], "split", down)
    pair = jnp.concatenate([before, pair, after], axis=2)
    (applied_rhs,) = call(apply_rhs, [(right_side.shape, F32)], pair)

    column = (part, nx)
    square = (nx, nx)
    stack = (planes,) + column
    mh, ml, ph, plo, qh, qlo, tail, cols = call(
        prepare,
        [((planes,) + square, BF16)] * 2 + [(square, BF16)] * 4 + [(column, F32), (stack, F32)],
        place,
        *blocks,
        pieces,
        smem=1,
    )

    zero = jnp.zeros(column, F32)
    held, out = zero, tail
    for t in range(depth - 1):
        came = lax.ppermute(out, "layer", [(t, t + 1)])
        if t < depth - 2:
            held, out = call(hop, [(column, F32)] * 2, held, came, tail, ph, plo)
    lower, top = call(turn, [(stack, F32), (column, F32)], held, came, cols, mh, ml)

    held, out = zero, top
    for t in range(depth - 1):
        came = lax.ppermute(out, "layer", [(depth - 1 - t, depth - 2 - t)])
        if t < depth - 2:
            held, out = call(hop, [(column, F32)] * 2, held, came, top, qh, qlo)
    swept, above = call(rise, [(stack, F32), (column, F32)], held, came, lower, mh, ml)

    up, down = neighbours(swept, "layer")
    behind = lax.ppermute(swept[-2:], "layer", up)
    ahead = lax.ppermute(swept[1:2], "layer", down)
    rows = width + 2 * EDGE
    packed = (planes + 4) * part
    vm = pl.BlockSpec(memory_space=pltpu.VMEM)
    windows = pl.pallas_call(
        pack,
        out_shape=jax.ShapeDtypeStruct((splits, rows, packed), F32),
        in_specs=[vm] * 4,
        out_specs=vm,
        scratch_shapes=[pltpu.VMEM((nx + 2 * EDGE, packed), F32)],
        name="pack",
    )(swept, behind, above, ahead)
    recv = lax.all_to_all(windows, "split", split_axis=0, concat_axis=0, tiled=True)

    where = jnp.stack(
        [own * width - EDGE, layer * planes - 2, splits * width, depth * planes]
    ).astype(jnp.int32)
    block = (right_side.shape, F32)
    total = depth * splits
    direction, image, applied_image, sums = call(
        images, [block] * 3 + [((total, ny), F32)], where, recv, pair, applied_rhs, smem=1
    )
    every = lax.all_to_all(sums, ("layer", "split"), split_axis=0, concat_axis=0, tiled=True)
    return tuple(
        call(
            finish, [block] * 2, every, direction, image, applied_image, right_side, applied_rhs
        )
    )


def solution(mesh):
    placed = (P("layer", "split", None), P("layer", "split", None), P("layer", None, "split"))
    return jax.shard_map(
        per_device,
        mesh=mesh,
        in_specs=placed,
        out_specs=(P("layer", "split", None), P("layer", "split", None)),
        check_vma=False,
    )
```

```python
import jax
import jax.numpy as jnp
from jax import lax
from jax.experimental import pallas as pl
from jax.experimental.pallas import tpu as pltpu
from jax.sharding import PartitionSpec as P

F32 = jnp.float32
BF16 = jnp.bfloat16
EDGE = 8


def split_parts(x):
    high = x.astype(BF16)
    return high, (x - high.astype(F32)).astype(BF16)


def dot_nt(a, b):
    return lax.dot_general(a, b, (((1,), (1,)), ((), ())), preferred_element_type=F32)


def apply_rows(rows, high, low):
    n = rows.shape[0]
    a, b = split_parts(rows)
    both = dot_nt(jnp.concatenate([a, b], axis=0), high)
    return both[:n] + both[n:] + dot_nt(a, low)


def product(a, b):
    ah, al = a
    bh, bl = b
    out = jnp.dot(ah, bh, preferred_element_type=F32)
    out = out + jnp.dot(ah, bl, preferred_element_type=F32)
    return out + jnp.dot(al, bh, preferred_element_type=F32)


def chain_product(pairs):
    while len(pairs) > 1:
        merged = [
            split_parts(product(pairs[i], pairs[i + 1])) for i in range(0, len(pairs) - 1, 2)
        ]
        if len(pairs) % 2:
            merged.append(pairs[-1])
        pairs = merged
    return pairs[0]


def near(x):
    return pltpu.with_memory_space_constraint(x, pltpu.VMEM)


def call(body, out, *args, smem=0, stay=True, scratch=()):
    vm = pl.BlockSpec(memory_space=pltpu.VMEM)
    specs = [pl.BlockSpec(memory_space=pltpu.SMEM)] * smem + [vm] * (len(args) - smem)
    shapes = [pltpu.VMEM(s, d) if stay else jax.ShapeDtypeStruct(s, d) for s, d in out]
    args = args[:smem] + tuple(near(x) for x in args[smem:])
    return pl.pallas_call(
        body,
        out_shape=shapes,
        in_specs=specs,
        out_specs=[vm] * len(shapes),
        scratch_shapes=scratch,
        name=body.__name__,
        compiler_params=pltpu.CompilerParams(vmem_limit_bytes=32 * 1024 * 1024),
    )(*args)


def prepare(place, *refs):
    count = place.shape[0]
    blocks = refs[:count]
    pieces, mh, ml, ph, plo, qh, qlo, tail, cols = refs[count:]
    planes, nx, width = blocks[0].shape
    for j in range(count):
        at = pl.multiple_of(place[j] * width, width)
        for k in range(planes):
            high, low = split_parts(blocks[j][k])
            mh[k, :, pl.ds(at, width)] = high
            ml[k, :, pl.ds(at, width)] = low
        cols[:, :, j * width : (j + 1) * width] = pieces[j]
    state = cols[0]
    for k in range(planes):
        if k:
            state = state + cols[k]
        state = apply_rows(state, mh[k], ml[k])
    tail[...] = state
    order = [(mh[k], ml[k]) for k in range(planes)]
    ph[...], plo[...] = chain_product(order[::-1])
    qh[...], qlo[...] = chain_product(order)


def hop(held, came, base, high, low, now, out):
    state = held[...] + came[...]
    now[...] = state
    out[...] = base[...] + apply_rows(state, high[...], low[...])


def turn(held, came, cols, mh, ml, lower, top):
    planes = cols.shape[0]
    state = held[...] + came[...]
    for k in range(planes):
        state = apply_rows(cols[k] + state, mh[k], ml[k])
        lower[k] = state
    for k in reversed(range(planes - 1)):
        state = lower[k] + apply_rows(state, mh[k], ml[k])
    top[...] = state


def rise(held, came, lower, mh, ml, direction, now):
    planes = lower.shape[0]
    state = held[...] + came[...]
    now[...] = state
    for k in reversed(range(planes)):
        state = lower[k] + apply_rows(state, mh[k], ml[k])
        direction[k] = state


def pack(direction, behind, above, ahead, out, tall):
    planes, ny, nx = direction.shape
    extended = jnp.concatenate([behind[...], direction[...], above[...][None], ahead[...]], axis=0)
    flat = extended.reshape((planes + 4) * ny, nx)
    tall[:EDGE] = jnp.zeros((EDGE, tall.shape[1]), F32)
    tall[EDGE + nx :] = jnp.zeros((EDGE, tall.shape[1]), F32)
    tall[EDGE : EDGE + nx] = flat.T
    count = out.shape[0]
    width = nx // count
    for j in range(count):
        out[j] = tall[j * width : j * width + width + 2 * EDGE]


def plane_stencil(below, here, above, diagonal):
    rows, ny = here.shape
    lane = lax.broadcasted_iota(jnp.int32, here.shape, 1)
    beside = below + above + pltpu.roll(here, 1, 0) + pltpu.roll(here, rows - 1, 0)
    beside = beside + jnp.where(lane > 0, pltpu.roll(here, 1, 1), 0.0)
    beside = beside + jnp.where(lane < ny - 1, pltpu.roll(here, ny - 1, 1), 0.0)
    return (6.0 + diagonal) * here - beside


def apply_rhs(extended, out):
    planes = out.shape[0]
    for k in range(planes):
        value = plane_stencil(
            extended[0, k], extended[0, k + 1], extended[0, k + 2], extended[1, k + 1]
        )
        out[k] = value[EDGE:-EDGE]


def images(where, recv, extended, applied_rhs, direction, image, applied_image, sums):
    planes = direction.shape[0]
    count, rows, packed = recv.shape
    part = packed // (planes + 4)
    depth = [
        jnp.concatenate([recv[j, :, p * part : (p + 1) * part] for j in range(count)], axis=1)
        for p in range(planes + 4)
    ]
    row = lax.broadcasted_iota(jnp.int32, depth[0].shape, 0) + where[0]
    inside_x = jnp.logical_and(row >= 0, row < where[2])
    made = {}
    for p in range(1, planes + 3):
        value = plane_stencil(depth[p - 1], depth[p], depth[p + 1], extended[1, p - 1])
        at = where[1] + p
        inside_z = jnp.logical_and(at >= 0, at < where[3])
        made[p] = jnp.where(jnp.logical_and(inside_x, inside_z), value, 0.0)
    totals = [jnp.zeros((EDGE, depth[0].shape[1]), F32) for _ in range(8)]
    for k in range(planes):
        p = k + 2
        twice = plane_stencil(made[p - 1], made[p], made[p + 1], extended[1, k + 1])[EDGE:-EDGE]
        once = made[p][EDGE:-EDGE]
        source = extended[0, k + 1][EDGE:-EDGE]
        about = applied_rhs[k]
        direction[k] = depth[p][EDGE:-EDGE]
        image[k] = once
        applied_image[k] = twice
        terms = (
            source * source,
            source * once,
            about * source,
            about * once + twice * source,
            twice * once,
            about * about,
            about * twice,
            twice * twice,
        )
        for i, term in enumerate(terms):
            totals[i] = totals[i] + jnp.sum(term.reshape(-1, EDGE, term.shape[1]), axis=0)
    lane = lax.broadcasted_iota(jnp.int32, sums.shape, 1)
    line = jnp.zeros(sums.shape, F32)
    for i, total in enumerate(totals):
        line = jnp.where(lane == i, jnp.sum(total), line)
    sums[...] = line


def finish(every, direction, image, applied_image, right_side, applied_rhs, solved, residual):
    total = jnp.sum(every[...], axis=0, keepdims=True)
    lane = lax.broadcasted_iota(jnp.int32, total.shape, 1)

    def pick(i):
        return jnp.sum(jnp.where(lane == i, total, 0.0), axis=1, keepdims=True)

    rr, ri, ar, cross, aii, arar, arai, aiai = [pick(i) for i in range(8)]
    alpha = rr / ri
    upper = ar - alpha * cross + alpha * alpha * aii
    under = arar - 2.0 * alpha * arai + alpha * alpha * aiai
    omega = upper / under
    for k in range(direction.shape[0]):
        middle = right_side[k] - alpha * image[k]
        tangent = applied_rhs[k] - alpha * applied_image[k]
        solved[k] = alpha * direction[k] + omega * middle
        residual[k] = middle - omega * tangent


def neighbours(x, axis):
    size = lax.axis_size(axis)
    up = [(i, i + 1) for i in range(size - 1)]
    down = [(i + 1, i) for i in range(size - 1)]
    return up, down


def per_device(right_side, diagonal, inverses):
    splits = lax.axis_size("split")
    depth = lax.axis_size("layer")
    own = lax.axis_index("split")
    layer = lax.axis_index("layer")
    planes, width, ny = right_side.shape
    nx = inverses.shape[1]
    part = ny // splits

    turned = jnp.swapaxes(right_side, 1, 2).reshape(planes, splits, part, width)
    pieces = lax.all_to_all(
        jnp.swapaxes(turned, 0, 1), "split", split_axis=0, concat_axis=0, tiled=True
    )

    pair = jnp.stack([right_side, diagonal])
    up, down = neighbours(pair, "layer")
    before = lax.ppermute(pair[:, -1:], "layer", up)
    after = lax.ppermute(pair[:, :1], "layer", down)
    pair = jnp.concatenate([before, pair, after], axis=1)
    up, down = neighbours(pair, "split")
    before = lax.ppermute(pair[:, :, -EDGE:], "split", up)
    after = lax.ppermute(pair[:, :, :EDGE], "split", down)
    pair = jnp.concatenate([before, pair, after], axis=2)
    (applied_rhs,) = call(apply_rhs, [(right_side.shape, F32)], pair)

    blocks = [inverses]
    offsets = [0]
    step = splits // 2
    while step:
        route = [(i, i ^ step) for i in range(splits)]
        blocks = blocks + [lax.ppermute(b, "split", route) for b in blocks]
        if len(blocks) == 2:
            blocks[1], pieces, pair, applied_rhs = lax.optimization_barrier(
                (blocks[1], pieces, pair, applied_rhs)
            )
        offsets = offsets + [o ^ step for o in offsets]
        step //= 2
    place = jnp.stack([own ^ o for o in offsets]).astype(jnp.int32)

    column = (part, nx)
    square = (nx, nx)
    stack = (planes,) + column
    mh, ml, ph, plo, qh, qlo, tail, cols = call(
        prepare,
        [((planes,) + square, BF16)] * 2 + [(square, BF16)] * 4 + [(column, F32), (stack, F32)],
        place,
        *blocks,
        pieces,
        smem=1,
    )

    zero = jnp.zeros(column, F32)
    held, out = zero, tail
    for t in range(depth - 1):
        came = lax.ppermute(out, "layer", [(t, t + 1)])
        if t < depth - 2:
            held, out = call(hop, [(column, F32)] * 2, held, came, tail, ph, plo)
    lower, top = call(turn, [(stack, F32), (column, F32)], held, came, cols, mh, ml)

    held, out = zero, top
    for t in range(depth - 1):
        came = lax.ppermute(out, "layer", [(depth - 1 - t, depth - 2 - t)])
        if t < depth - 2:
            held, out = call(hop, [(column, F32)] * 2, held, came, top, qh, qlo)
    swept, above = call(rise, [(stack, F32), (column, F32)], held, came, lower, mh, ml)

    up, down = neighbours(swept, "layer")
    behind = lax.ppermute(swept[-2:], "layer", up)
    ahead = lax.ppermute(swept[1:2], "layer", down)
    rows = width + 2 * EDGE
    packed = (planes + 4) * part
    (windows,) = call(
        pack,
        [((splits, rows, packed), F32)],
        swept,
        behind,
        above,
        ahead,
        scratch=[pltpu.VMEM((nx + 2 * EDGE, packed), F32)],
    )
    recv = lax.all_to_all(windows, "split", split_axis=0, concat_axis=0, tiled=True)

    where = jnp.stack(
        [own * width - EDGE, layer * planes - 2, splits * width, depth * planes]
    ).astype(jnp.int32)
    block = (right_side.shape, F32)
    total = depth * splits
    direction, image, applied_image, sums = call(
        images, [block] * 3 + [((total, ny), F32)], where, recv, pair, applied_rhs, smem=1
    )
    every = lax.all_to_all(sums, ("layer", "split"), split_axis=0, concat_axis=0, tiled=True)
    return tuple(
        call(
            finish,
            [block] * 2,
            every,
            direction,
            image,
            applied_image,
            right_side,
            applied_rhs,
            stay=False,
        )
    )


def solution(mesh):
    placed = (P("layer", "split", None), P("layer", "split", None), P("layer", None, "split"))
    return jax.shard_map(
        per_device,
        mesh=mesh,
        in_specs=placed,
        out_specs=(P("layer", "split", None), P("layer", "split", None)),
        check_vma=False,
    )
```

```python
import jax
import jax.numpy as jnp
from jax import lax
from jax.experimental import pallas as pl
from jax.experimental.pallas import tpu as pltpu
from jax.sharding import PartitionSpec as P

F32 = jnp.float32
BF16 = jnp.bfloat16
EDGE = 8


def split_parts(x):
    high = x.astype(BF16)
    return high, (x - high.astype(F32)).astype(BF16)


def dot_nt(a, b):
    return lax.dot_general(a, b, (((1,), (1,)), ((), ())), preferred_element_type=F32)


def apply_rows(rows, high, low):
    n = rows.shape[0]
    a, b = split_parts(rows)
    both = dot_nt(jnp.concatenate([a, b], axis=0), high)
    return both[:n] + both[n:] + dot_nt(a, low)


def product(a, b):
    ah, al = a
    bh, bl = b
    out = jnp.dot(ah, bh, preferred_element_type=F32)
    out = out + jnp.dot(ah, bl, preferred_element_type=F32)
    return out + jnp.dot(al, bh, preferred_element_type=F32)


def chain_product(pairs):
    while len(pairs) > 1:
        merged = [
            split_parts(product(pairs[i], pairs[i + 1])) for i in range(0, len(pairs) - 1, 2)
        ]
        if len(pairs) % 2:
            merged.append(pairs[-1])
        pairs = merged
    return pairs[0]


def near(x):
    return pltpu.with_memory_space_constraint(x, pltpu.VMEM)


def call(body, out, *args, smem=0, stay=True, scratch=()):
    vm = pl.BlockSpec(memory_space=pltpu.VMEM)
    specs = [pl.BlockSpec(memory_space=pltpu.SMEM)] * smem + [vm] * (len(args) - smem)
    shapes = [pltpu.VMEM(s, d) if stay else jax.ShapeDtypeStruct(s, d) for s, d in out]
    args = args[:smem] + tuple(near(x) for x in args[smem:])
    return pl.pallas_call(
        body,
        out_shape=shapes,
        in_specs=specs,
        out_specs=[vm] * len(shapes),
        scratch_shapes=scratch,
        name=body.__name__,
        compiler_params=pltpu.CompilerParams(vmem_limit_bytes=32 * 1024 * 1024),
    )(*args)


def prepare(place, *refs):
    count = place.shape[0]
    blocks = refs[:count]
    pieces, mh, ml, ph, plo, tail, cols = refs[count:]
    planes, nx, width = blocks[0].shape
    for j in range(count):
        at = pl.multiple_of(place[j] * width, width)
        for k in range(planes):
            high, low = split_parts(blocks[j][k])
            mh[k, :, pl.ds(at, width)] = high
            ml[k, :, pl.ds(at, width)] = low
        cols[:, :, j * width : (j + 1) * width] = pieces[j]
    state = cols[0]
    for k in range(planes):
        if k:
            state = state + cols[k]
        state = apply_rows(state, mh[k], ml[k])
    tail[...] = state
    order = [(mh[k], ml[k]) for k in range(planes)]
    ph[...], plo[...] = chain_product(order[::-1])


def prepare_up(mh, ml, qh, qlo):
    order = [(mh[k], ml[k]) for k in range(mh.shape[0])]
    qh[...], qlo[...] = chain_product(order)


def hop(held, came, base, high, low, now, out):
    state = held[...] + came[...]
    now[...] = state
    out[...] = base[...] + apply_rows(state, high[...], low[...])


def turn(held, came, cols, mh, ml, lower, top):
    planes = cols.shape[0]
    state = held[...] + came[...]
    for k in range(planes):
        state = apply_rows(cols[k] + state, mh[k], ml[k])
        lower[k] = state
    for k in reversed(range(planes - 1)):
        state = lower[k] + apply_rows(state, mh[k], ml[k])
    top[...] = state


def rise(held, came, lower, mh, ml, direction, now):
    planes = lower.shape[0]
    state = held[...] + came[...]
    now[...] = state
    for k in reversed(range(planes)):
        state = lower[k] + apply_rows(state, mh[k], ml[k])
        direction[k] = state


def pack(direction, behind, above, ahead, out, tall):
    planes, ny, nx = direction.shape
    extended = jnp.concatenate([behind[...], direction[...], above[...][None], ahead[...]], axis=0)
    flat = extended.reshape((planes + 4) * ny, nx)
    tall[:EDGE] = jnp.zeros((EDGE, tall.shape[1]), F32)
    tall[EDGE + nx :] = jnp.zeros((EDGE, tall.shape[1]), F32)
    tall[EDGE : EDGE + nx] = flat.T
    count = out.shape[0]
    width = nx // count
    for j in range(count):
        out[j] = tall[j * width : j * width + width + 2 * EDGE]


def plane_stencil(below, here, above, diagonal):
    rows, ny = here.shape
    lane = lax.broadcasted_iota(jnp.int32, here.shape, 1)
    beside = below + above + pltpu.roll(here, 1, 0) + pltpu.roll(here, rows - 1, 0)
    beside = beside + jnp.where(lane > 0, pltpu.roll(here, 1, 1), 0.0)
    beside = beside + jnp.where(lane < ny - 1, pltpu.roll(here, ny - 1, 1), 0.0)
    return (6.0 + diagonal) * here - beside


def apply_rhs(extended, out):
    planes = out.shape[0]
    for k in range(planes):
        value = plane_stencil(
            extended[0, k], extended[0, k + 1], extended[0, k + 2], extended[1, k + 1]
        )
        out[k] = value[EDGE:-EDGE]


def images(where, recv, extended, applied_rhs, direction, image, applied_image, sums):
    planes = direction.shape[0]
    count, rows, packed = recv.shape
    part = packed // (planes + 4)
    depth = [
        jnp.concatenate([recv[j, :, p * part : (p + 1) * part] for j in range(count)], axis=1)
        for p in range(planes + 4)
    ]
    row = lax.broadcasted_iota(jnp.int32, depth[0].shape, 0) + where[0]
    inside_x = jnp.logical_and(row >= 0, row < where[2])
    made = {}
    for p in range(1, planes + 3):
        value = plane_stencil(depth[p - 1], depth[p], depth[p + 1], extended[1, p - 1])
        at = where[1] + p
        inside_z = jnp.logical_and(at >= 0, at < where[3])
        made[p] = jnp.where(jnp.logical_and(inside_x, inside_z), value, 0.0)
    totals = [jnp.zeros((EDGE, depth[0].shape[1]), F32) for _ in range(8)]
    for k in range(planes):
        p = k + 2
        twice = plane_stencil(made[p - 1], made[p], made[p + 1], extended[1, k + 1])[EDGE:-EDGE]
        once = made[p][EDGE:-EDGE]
        source = extended[0, k + 1][EDGE:-EDGE]
        about = applied_rhs[k]
        direction[k] = depth[p][EDGE:-EDGE]
        image[k] = once
        applied_image[k] = twice
        terms = (
            source * source,
            source * once,
            about * source,
            about * once + twice * source,
            twice * once,
            about * about,
            about * twice,
            twice * twice,
        )
        for i, term in enumerate(terms):
            totals[i] = totals[i] + jnp.sum(term.reshape(-1, EDGE, term.shape[1]), axis=0)
    lane = lax.broadcasted_iota(jnp.int32, sums.shape, 1)
    line = jnp.zeros(sums.shape, F32)
    for i, total in enumerate(totals):
        line = jnp.where(lane == i, jnp.sum(total), line)
    sums[...] = line


def finish(every, direction, image, applied_image, right_side, applied_rhs, solved, residual):
    total = jnp.sum(every[...], axis=0, keepdims=True)
    lane = lax.broadcasted_iota(jnp.int32, total.shape, 1)

    def pick(i):
        return jnp.sum(jnp.where(lane == i, total, 0.0), axis=1, keepdims=True)

    rr, ri, ar, cross, aii, arar, arai, aiai = [pick(i) for i in range(8)]
    alpha = rr / ri
    upper = ar - alpha * cross + alpha * alpha * aii
    under = arar - 2.0 * alpha * arai + alpha * alpha * aiai
    omega = upper / under
    for k in range(direction.shape[0]):
        middle = right_side[k] - alpha * image[k]
        tangent = applied_rhs[k] - alpha * applied_image[k]
        solved[k] = alpha * direction[k] + omega * middle
        residual[k] = middle - omega * tangent


def neighbours(x, axis):
    size = lax.axis_size(axis)
    up = [(i, i + 1) for i in range(size - 1)]
    down = [(i + 1, i) for i in range(size - 1)]
    return up, down


def per_device(right_side, diagonal, inverses):
    splits = lax.axis_size("split")
    depth = lax.axis_size("layer")
    own = lax.axis_index("split")
    layer = lax.axis_index("layer")
    planes, width, ny = right_side.shape
    nx = inverses.shape[1]
    part = ny // splits

    turned = jnp.swapaxes(right_side, 1, 2).reshape(planes, splits, part, width)
    pieces = lax.all_to_all(
        jnp.swapaxes(turned, 0, 1), "split", split_axis=0, concat_axis=0, tiled=True
    )

    pair = jnp.stack([right_side, diagonal])
    up, down = neighbours(pair, "layer")
    before = lax.ppermute(pair[:, -1:], "layer", up)
    after = lax.ppermute(pair[:, :1], "layer", down)
    pair = jnp.concatenate([before, pair, after], axis=1)
    up, down = neighbours(pair, "split")
    before = lax.ppermute(pair[:, :, -EDGE:], "split", up)
    after = lax.ppermute(pair[:, :, :EDGE], "split", down)
    pair = jnp.concatenate([before, pair, after], axis=2)
    (applied_rhs,) = call(apply_rhs, [(right_side.shape, F32)], pair)

    blocks = [inverses]
    offsets = [0]
    step = splits // 2
    while step:
        route = [(i, i ^ step) for i in range(splits)]
        blocks = blocks + [lax.ppermute(b, "split", route) for b in blocks]
        if len(blocks) == 2:
            blocks[1], pieces, pair, applied_rhs = lax.optimization_barrier(
                (blocks[1], pieces, pair, applied_rhs)
            )
        offsets = offsets + [o ^ step for o in offsets]
        step //= 2
    place = jnp.stack([own ^ o for o in offsets]).astype(jnp.int32)

    column = (part, nx)
    square = (nx, nx)
    stack = (planes,) + column
    mh, ml, ph, plo, tail, cols = call(
        prepare,
        [((planes,) + square, BF16)] * 2 + [(square, BF16)] * 2 + [(column, F32), (stack, F32)],
        place,
        *blocks,
        pieces,
        smem=1,
    )

    qh, qlo = call(prepare_up, [(square, BF16)] * 2, mh, ml)

    zero = jnp.zeros(column, F32)
    held, out = zero, tail
    for t in range(depth - 1):
        came = lax.ppermute(out, "layer", [(t, t + 1)])
        if t == 0:
            came, qh, qlo = lax.optimization_barrier((came, qh, qlo))
        if t < depth - 2:
            held, out = call(hop, [(column, F32)] * 2, held, came, tail, ph, plo)
    lower, top = call(turn, [(stack, F32), (column, F32)], held, came, cols, mh, ml)

    held, out = zero, top
    for t in range(depth - 1):
        came = lax.ppermute(out, "layer", [(depth - 1 - t, depth - 2 - t)])
        if t < depth - 2:
            held, out = call(hop, [(column, F32)] * 2, held, came, top, qh, qlo)
    swept, above = call(rise, [(stack, F32), (column, F32)], held, came, lower, mh, ml)

    up, down = neighbours(swept, "layer")
    behind = lax.ppermute(swept[-2:], "layer", up)
    ahead = lax.ppermute(swept[1:2], "layer", down)
    rows = width + 2 * EDGE
    packed = (planes + 4) * part
    (windows,) = call(
        pack,
        [((splits, rows, packed), F32)],
        swept,
        behind,
        above,
        ahead,
        scratch=[pltpu.VMEM((nx + 2 * EDGE, packed), F32)],
    )
    recv = lax.all_to_all(windows, "split", split_axis=0, concat_axis=0, tiled=True)

    where = jnp.stack(
        [own * width - EDGE, layer * planes - 2, splits * width, depth * planes]
    ).astype(jnp.int32)
    block = (right_side.shape, F32)
    total = depth * splits
    direction, image, applied_image, sums = call(
        images, [block] * 3 + [((total, ny), F32)], where, recv, pair, applied_rhs, smem=1
    )
    every = lax.all_to_all(sums, ("layer", "split"), split_axis=0, concat_axis=0, tiled=True)
    return tuple(
        call(
            finish,
            [block] * 2,
            every,
            direction,
            image,
            applied_image,
            right_side,
            applied_rhs,
            stay=False,
        )
    )


def solution(mesh):
    placed = (P("layer", "split", None), P("layer", "split", None), P("layer", None, "split"))
    return jax.shard_map(
        per_device,
        mesh=mesh,
        in_specs=placed,
        out_specs=(P("layer", "split", None), P("layer", "split", None)),
        check_vma=False,
    )
```
